32 devices in a mesh: lon: 8 (over y, x, core), dp: 4 (over z).
Axes of the slice: x: 2, y: 2, z: 4, core: 2. Of those that a mesh axis runs over, the one named last changes fastest.
Arguments:
- inputs: bfloat16 [4, 32, 384, 256], P('dp', None, 'lon'), may hold values from -6 to 6
- pre_act: bfloat16 [4, 32, 384, 256], P('dp', None, 'lon'), may hold values from -6 to 6
- cotangent: bfloat16 [4, 32, 384, 256], P('dp', None, 'lon'), may hold values from -6 to 6
- first_weight: bfloat16 [2304, 256], replicated, may hold values from -0.125 to 0.125
- second_weight: bfloat16 [2304, 256], replicated, may hold values from -0.125 to 0.125
Outputs:
- input_gradient_array: bfloat16 [4, 32, 384, 256], P('dp', None, 'lon')
- first_weight_gradient: float32 [589824], P(('lon', 'dp'))
- second_weight_gradient: float32 [589824], P(('lon', 'dp'))
The draws below stay inside these ranges and needn't reach their ends.
All inputs are finite; a program needn't handle non-finite values.
Results may differ from the reference program's by a relative error of at most 0.0049.
Values may be sent and summed in bfloat16 or wider, within the bound.
No kernel may reach another device: no remote copies, remote signals or barrier semaphores. Data moves between devices by JAX's collectives and lax.ppermute only.
A program may use at most 64 MiB of HBM per device.

```python
import jax
import jax.numpy as jnp

C = 256
FIRST_SPREAD = 12
SECOND_SPREAD = 18
LAT = 32
NLON = 384
SAMPLES = 4


def shard_levels(stream_key, shape, split, least, largest):
    def one(axis_at, blocks):
        steps = jax.random.uniform(jax.random.fold_in(jax.random.fold_in(stream_key, 6), axis_at), (blocks,), jnp.float32, least / len(split), largest / len(split))
        return jnp.repeat(jnp.exp(steps), shape[axis_at] // blocks).reshape((-1,) + (1,) * (len(shape) - axis_at - 1))

    level = one(*split[0])
    for cut in split[1:]:
        level = level * one(*cut)
    return level


def bell_draw(key, extent, scale, bound, cuts=(), held_as=jnp.bfloat16):
    result = scale * jax.random.normal(key, extent, jnp.float32)
    if cuts:
        result = result * shard_levels(key, extent, cuts, -0.22, 0.18)
    return jnp.clip(result, -bound, bound).astype(held_as)


def setup_inputs(seed: int = 0) -> dict:
    seeds = jax.random.split(jax.random.key(seed), 6)
    return {
        "inputs": bell_draw(seeds[0], (SAMPLES, LAT, NLON, C), 1.0, 6.0, ((0, 4), (2, 8))),
        "pre_act": bell_draw(seeds[1], (SAMPLES, LAT, NLON, C), 1.0, 6.0, ((0, 4), (2, 8))),
        "cotangent": bell_draw(seeds[2], (SAMPLES, LAT, NLON, C), 1.0, 6.0, ((0, 4), (2, 8))),
        "first_weight": bell_draw(seeds[3], (9 * C, C), (9 * C) ** -0.5, 0.125),
        "second_weight": bell_draw(seeds[4], (9 * C, C), (9 * C) ** -0.5, 0.125),
    }


def lat_move(values, offset):
    rows = values.shape[1]
    if abs(offset) >= rows:
        return jnp.zeros_like(values)
    if offset == 0:
        return values
    blank = jnp.zeros_like(values[:, :abs(offset)])
    if offset > 0:
        return jnp.concatenate([values[:, offset:], blank], axis=1)
    return jnp.concatenate([blank, values[:, :rows + offset]], axis=1)


def shifted(values, dilation, tap, direction):
    lat_off = direction * (tap // 3 - 1) * dilation
    lon_off = direction * (tap % 3 - 1) * dilation
    return lat_move(jnp.roll(values, -lon_off, axis=2), lat_off)


def kernel_weight_gradient(source, dilation, upstream):
    chans = upstream.shape[3]
    flat_up = upstream.reshape(-1, chans)
    blocks = []
    for tap in range(9):
        moved = shifted(source, dilation, tap, 1).reshape(-1, source.shape[3])
        blocks.append(jnp.dot(moved.T, flat_up, preferred_element_type=jnp.float32))
    return jnp.concatenate(blocks, axis=0)


def gradient_wrt_input(upstream, dilation, weights):
    chans = weights.shape[1]
    total = jnp.zeros((upstream.shape[0] * upstream.shape[1] * upstream.shape[2], weights.shape[1]), jnp.float32)
    for tap in range(9):
        moved = shifted(upstream, dilation, tap, -1).reshape(-1, chans)
        block = weights[tap * chans:(tap + 1) * chans]
        total = total + jnp.dot(moved, block.T, preferred_element_type=jnp.float32)
    return total.reshape(upstream.shape)


def reference(inputs, pre_act, cotangent, first_weight, second_weight):
    norm_factor = float(SAMPLES * LAT * NLON) ** -0.5
    hidden_activation = jnp.maximum(pre_act, jnp.zeros_like(pre_act))
    second_weight_gradient = (kernel_weight_gradient(hidden_activation, SECOND_SPREAD, cotangent) * norm_factor).reshape(-1)
    hidden_gradient = gradient_wrt_input(cotangent, SECOND_SPREAD, second_weight)
    partial_gradient = jnp.where(pre_act > 0, hidden_gradient, jnp.float32(0.0)).astype(jnp.bfloat16)
    first_weight_gradient = (kernel_weight_gradient(inputs, FIRST_SPREAD, partial_gradient) * norm_factor).reshape(-1)
    input_gradient_array = gradient_wrt_input(partial_gradient, FIRST_SPREAD, first_weight).astype(jnp.bfloat16)
    return input_gradient_array, first_weight_gradient, second_weight_gradient
```

```python
import functools

import jax
import jax.numpy as jnp
from jax import lax
from jax.experimental import pallas as pl
from jax.experimental.pallas import tpu as pltpu
from jax.sharding import PartitionSpec as P

FIRST_SPREAD = 12
SECOND_SPREAD = 18
FIRST_PAD = 4
SECOND_PAD = 2
BF16 = jnp.bfloat16
F32 = jnp.float32


def build_views(src, low, high, views, spread, pad, plus, minus):
    rows, cols, chans = src.shape
    blank = jnp.zeros((pad * cols, 3 * chans), BF16)
    if pad:
        views[: pad * cols, :] = blank
        views[(pad + rows) * cols :, :] = blank
    for p in range(rows):
        at = pl.ds((pad + p) * cols, cols)
        row = src[p]
        views[at, chans : 2 * chans] = row
        row = row.astype(F32)
        strip = pl.ds(p * spread, spread)
        upper = high[strip, :].astype(F32)
        lower = low[strip, :].astype(F32)
        views[at, plus * chans : (plus + 1) * chans] = jnp.concatenate(
            [row[spread:], upper], axis=0
        ).astype(BF16)
        views[at, minus * chans : (minus + 1) * chans] = jnp.concatenate(
            [lower, row[: cols - spread]], axis=0
        ).astype(BF16)


def transpose_taps(weight, turned):
    chans = weight.shape[1]
    for k in range(9):
        turned[k * chans : (k + 1) * chans, :] = weight[k * chans : (k + 1) * chans, :].T


def input_side(views, turned, total, rows, cols, spread, pad):
    chans = total.shape[1]
    part = (rows - spread) * cols
    first = pad * cols
    total[...] = jnp.dot(
        views[first : first + rows * cols, :],
        turned[3 * chans : 6 * chans, :],
        preferred_element_type=F32,
    )
    ahead = (pad + spread) * cols
    total[:part, :] += jnp.dot(
        views[ahead : ahead + part, :], turned[: 3 * chans, :], preferred_element_type=F32
    )
    total[spread * cols :, :] += jnp.dot(
        views[first : first + part, :], turned[6 * chans :, :], preferred_element_type=F32
    )


def weight_side(still, views, rows, cols, spread, pad, direction, norm, store):
    block = rows - spread + pad
    chans = still.shape[0]
    ahead = (0, block * cols, (pad + spread) * cols)
    middle = (0, rows * cols, pad * cols)
    behind = ((rows - block) * cols, rows * cols, 0)
    order = (ahead, middle, behind) if direction < 0 else (behind, middle, ahead)
    for r, (low, high, start) in enumerate(order):
        product = norm * jnp.dot(
            still[:, low:high], views[start : start + high - low, :], preferred_element_type=F32
        )
        for c in range(3):
            store(3 * r + c, product[:, c * chans : (c + 1) * chans])


def hand_out(gradient, keep, send, segments):
    size = gradient.shape[0] // segments
    place = lax.axis_index("lon")
    core = lax.rem(place, 2)
    chip = place // 2
    for m in range(segments // 2):
        pair = 2 * lax.bitwise_xor(chip, m)
        mine = pl.ds(pl.multiple_of((pair + core) * size, size), size)
        other = pl.ds(pl.multiple_of((pair + 1 - core) * size, size), size)
        keep[m * size : (m + 1) * size, :] = gradient[mine, :]
        send[m * size : (m + 1) * size, :] = gradient[other, :]


def second_kernel(
    norm, segments, pre, cot, low, high, weight, keep, send, local, edge_low, edge_high,
    views, turned, still, total, gradient,
):
    rows, cols, chans = pre.shape
    spread, pad = SECOND_SPREAD, SECOND_PAD
    build_views(cot, low, high, views, spread, pad, 0, 2)
    transpose_taps(weight, turned)
    flat = pre[...].reshape(rows * cols, chans)
    still[...] = jnp.maximum(flat, jnp.zeros_like(flat)).T
    input_side(views, turned, total, rows, cols, spread, pad)
    width = FIRST_SPREAD
    for p in range(rows):
        value = jnp.where(
            pre[p].astype(F32) > 0, total[p * cols : (p + 1) * cols, :], jnp.float32(0.0)
        )
        local[p] = value.astype(BF16)
        edge_low[p * width : (p + 1) * width, :] = value[:width].astype(BF16)
        edge_high[p * width : (p + 1) * width, :] = value[cols - width :].astype(BF16)

    def store(k, block):
        gradient[k * chans : (k + 1) * chans, :] = block.astype(BF16)

    weight_side(still, views, rows, cols, spread, pad, -1, norm, store)
    hand_out(gradient, keep, send, segments)


def first_weight_kernel(
    norm, segments, inputs, low, high, local, keep, send, views, still, gradient
):
    rows, cols, chans = inputs.shape
    spread, pad = FIRST_SPREAD, FIRST_PAD
    build_views(inputs, low, high, views, spread, pad, 2, 0)
    still[...] = local[...].reshape(rows * cols, chans).T

    def store(k, block):
        gradient[k * chans : (k + 1) * chans, :] = block.astype(BF16).T

    weight_side(still, views, rows, cols, spread, pad, 1, norm, store)
    hand_out(gradient, keep, send, segments)


def first_input_kernel(local, low, high, weight, out, views, turned, total):
    rows, cols, chans = local.shape
    build_views(local, low, high, views, FIRST_SPREAD, 0, 0, 2)
    transpose_taps(weight, turned)
    input_side(views, turned, total, rows, cols, FIRST_SPREAD, 0)
    out[...] = total[...].astype(BF16).reshape(rows, cols, chans)


def call(kernel, outs, scratch, *operands):
    whole = pl.BlockSpec(memory_space=pltpu.VMEM)
    return pl.pallas_call(
        kernel,
        out_shape=[jax.ShapeDtypeStruct(s, BF16) for s in outs],
        in_specs=[whole] * len(operands),
        out_specs=[whole] * len(outs),
        scratch_shapes=[pltpu.VMEM(s, t) for s, t in scratch],
        compiler_params=pltpu.CompilerParams(vmem_limit_bytes=40 * 2**20),
    )(*operands)


def ring(axis, step):
    count = lax.axis_size(axis)
    return [(i, (i + step) % count) for i in range(count)]


def swap(axis, mask):
    return [(i, i ^ mask) for i in range(lax.axis_size(axis))]


def exchange_edges(low_edge, high_edge):
    low = lax.ppermute(high_edge, "lon", ring("lon", 1))
    high = lax.ppermute(low_edge, "lon", ring("lon", -1))
    return low, high


def edges_of(field, width):
    cols, chans = field.shape[1:]
    return (
        field[:, :width].reshape(-1, chans),
        field[:, cols - width :].reshape(-1, chans),
    )


def reduce_partials(keep, send):
    chips = lax.axis_size("lon") // 2
    parts = lax.axis_size("dp")
    chans = keep.shape[1]
    received = lax.ppermute(send, "lon", swap("lon", 1))
    paired = (keep.astype(F32) + received.astype(F32)).astype(BF16).reshape(chips, -1, chans)
    arrived = [lax.ppermute(paired[m], "lon", swap("lon", 2 * m)) for m in range(1, chips)]
    level = sum((a.astype(F32) for a in arrived), paired[0].astype(F32))
    level = level.reshape(parts, -1, chans)
    me = lax.axis_index("dp")
    own = lax.dynamic_index_in_dim(level, me, 0, keepdims=False)
    pieces = [
        lax.dynamic_index_in_dim(level, me ^ m, 0, keepdims=False).astype(BF16)
        for m in range(1, parts)
    ]
    arrived = [lax.ppermute(pieces[m - 1], "dp", swap("dp", m)) for m in range(1, parts)]
    return sum((a.astype(F32) for a in arrived), own).reshape(-1)


def local(inputs, pre_act, cotangent, first_weight, second_weight):
    shape = inputs.shape
    inputs, pre_act, cotangent = (a.reshape(a.shape[1:]) for a in (inputs, pre_act, cotangent))
    rows, cols, chans = inputs.shape
    segments = lax.axis_size("lon")
    cells = rows * cols
    norm = float(shape[0] * cells * segments * lax.axis_size("dp")) ** -0.5
    taps = first_weight.shape[0]
    cot_low, cot_high = exchange_edges(*edges_of(cotangent, SECOND_SPREAD))
    in_low, in_high = exchange_edges(*edges_of(inputs, FIRST_SPREAD))
    half = (taps // 2, chans)
    edge = (rows * FIRST_SPREAD, chans)
    keep, send, local_grad, edge_low, edge_high = call(
        functools.partial(second_kernel, norm, segments),
        [half, half, (rows, cols, chans), edge, edge],
        [
            (((rows + 2 * SECOND_PAD) * cols, 3 * chans), BF16),
            ((taps, chans), BF16),
            ((chans, cells), BF16),
            ((cells, chans), F32),
            ((taps, chans), BF16),
        ],
        pre_act, cotangent, cot_low, cot_high, second_weight,
    )
    grad_low, grad_high = exchange_edges(edge_low, edge_high)
    second = reduce_partials(keep, send)
    keep, send = call(
        functools.partial(first_weight_kernel, norm, segments),
        [half, half],
        [
            (((rows + 2 * FIRST_PAD) * cols, 3 * chans), BF16),
            ((chans, cells), BF16),
            ((taps, chans), BF16),
        ],
        inputs, in_low, in_high, local_grad,
    )
    first = reduce_partials(keep, send)
    (input_gradient,) = call(
        first_input_kernel,
        [(rows, cols, chans)],
        [
            ((cells, 3 * chans), BF16),
            ((taps, chans), BF16),
            ((cells, chans), F32),
        ],
        local_grad, grad_low, grad_high, first_weight,
    )
    return input_gradient.reshape(shape), first, second


def solution(mesh):
    field = P("dp", None, "lon", None)
    return jax.shard_map(
        local,
        mesh=mesh,
        in_specs=(field, field, field, P(), P()),
        out_specs=(field, P(("lon", "dp")), P(("lon", "dp"))),
        check_vma=False,
    )
```

```python
import functools

import jax
import jax.numpy as jnp
from jax import lax
from jax.experimental import pallas as pl
from jax.experimental.pallas import tpu as pltpu
from jax.sharding import PartitionSpec as P


FIRST_SPREAD = 12
SECOND_SPREAD = 18
FIRST_PAD = 4
SECOND_PAD = 2
BF16 = jnp.bfloat16
F32 = jnp.float32


def moved_rows(row, low, high, spread):
    cols = row.shape[0]
    return (
        jnp.concatenate([row[spread:], high], axis=0).astype(BF16),
        jnp.concatenate([low, row[: cols - spread]], axis=0).astype(BF16),
    )


def build_views(src, low, high, views, spread, pad, plus, minus):
    rows, cols, chans = src.shape
    if pad:
        blank = jnp.zeros((pad * cols, 3 * chans), BF16)
        views[: pad * cols, :] = blank
        views[(pad + rows) * cols :, :] = blank
    for p in range(rows):
        at = pl.ds((pad + p) * cols, cols)
        row = src[p]
        views[at, chans : 2 * chans] = row
        row = row.astype(F32)
        if low is None:
            upper = lower = jnp.zeros((spread, chans), F32)
        else:
            strip = pl.ds(p * spread, spread)
            upper = high[strip, :].astype(F32)
            lower = low[strip, :].astype(F32)
        ahead, behind = moved_rows(row, lower, upper, spread)
        views[at, plus * chans : (plus + 1) * chans] = ahead
        views[at, minus * chans : (minus + 1) * chans] = behind


def transpose_taps(weight, turned):
    chans = weight.shape[1]
    for k in range(9):
        turned[k * chans : (k + 1) * chans, :] = weight[k * chans : (k + 1) * chans, :].T


def input_side(views, turned, total, rows, cols, spread, pad):
    part = (rows - spread) * cols
    first = pad * cols
    third = turned.shape[0] // 3
    total[...] = jnp.dot(
        views[first : first + rows * cols, :],
        turned[third : 2 * third, :],
        preferred_element_type=F32,
    )
    ahead = (pad + spread) * cols
    total[:part, :] += jnp.dot(
        views[ahead : ahead + part, :], turned[:third, :], preferred_element_type=F32
    )
    total[spread * cols :, :] += jnp.dot(
        views[first : first + part, :], turned[2 * third :, :], preferred_element_type=F32
    )


def tap_rows(rows, cols, spread, pad, direction):
    block = rows - spread + pad
    ahead = (0, block * cols, (pad + spread) * cols)
    middle = (0, rows * cols, pad * cols)
    behind = ((rows - block) * cols, rows * cols, 0)
    return (ahead, middle, behind) if direction < 0 else (behind, middle, ahead)


def product(still, views, span):
    low, high, start = span
    return jnp.dot(
        still[:, low:high], views[start : start + high - low, :], preferred_element_type=F32
    )


def place_tap(gradient, k, block):
    chans = block.shape[0]
    half = chans // 2
    for h in range(2):
        at = pl.ds(2 * k * chans + h, chans, stride=2)
        gradient[at, :] = block[:, h * half : (h + 1) * half]


def hand_out(gradient, keep, send, segments):
    size = gradient.shape[0] // segments
    place = lax.axis_index("lon")
    core = lax.rem(place, 2)
    chip = place // 2
    for m in range(segments // 2):
        pair = 2 * lax.bitwise_xor(chip, m)
        mine = pl.ds(pl.multiple_of((pair + core) * size, size), size)
        other = pl.ds(pl.multiple_of((pair + 1 - core) * size, size), size)
        keep[m * size : (m + 1) * size, :] = gradient[mine, :].astype(BF16)
        send[m * size : (m + 1) * size, :] = gradient[other, :].astype(BF16)


def second_early_kernel(pre, cot, weight, total, taps, low_still, high_still, turned, views, still):
    rows, cols, chans = pre.shape
    spread, pad = SECOND_SPREAD, SECOND_PAD
    build_views(cot, None, None, views, spread, pad, 0, 2)
    transpose_taps(weight, turned)
    hidden = pre[...]
    hidden = jnp.maximum(hidden, jnp.zeros_like(hidden))
    still[...] = hidden.reshape(rows * cols, chans).T
    half = cols // 2
    low_still[...] = hidden[:, :half].reshape(rows * half, chans).T
    high_still[...] = hidden[:, half:].reshape(rows * half, chans).T
    input_side(views, turned, total, rows, cols, spread, pad)
    for r, span in enumerate(tap_rows(rows, cols, spread, pad, -1)):
        value = product(still, views, span)
        for c in range(3):
            k = 3 * r + c
            taps[k * chans : (k + 1) * chans, :] = value[:, c * chans : (c + 1) * chans]


def second_late_kernel(
    norm, segments, pre, low, high, early, taps, low_still, high_still, turned,
    keep, send, local, edge_low, edge_high, low_views, high_views, low_total, high_total, gradient,
):
    rows, cols, chans = pre.shape
    spread, pad = SECOND_SPREAD, SECOND_PAD
    half = cols // 2
    blank = jnp.zeros((pad * half, chans), BF16)
    for views in (low_views, high_views):
        views[: pad * half, :] = blank
        views[(pad + rows) * half :, :] = blank
    gap = jnp.zeros((half - spread, chans), F32)
    for p in range(0, rows, 2):
        at = pl.ds((pad + p) * half, 2 * half)
        lower = [low[q * spread : (q + 1) * spread, :].astype(F32) for q in (p, p + 1)]
        upper = [high[q * spread : (q + 1) * spread, :].astype(F32) for q in (p, p + 1)]
        low_views[at, :] = jnp.concatenate([lower[0], gap, lower[1], gap], axis=0).astype(BF16)
        high_views[at, :] = jnp.concatenate([gap, upper[0], gap, upper[1]], axis=0).astype(BF16)

    part = (rows - spread) * half
    first = pad * half
    ahead = (pad + spread) * half
    for views, total, c in ((low_views, low_total, 2), (high_views, high_total, 0)):

        def matrix(r):
            k = 3 * r + c
            return turned[k * chans : (k + 1) * chans, :]

        total[...] = jnp.dot(
            views[first : first + rows * half, :], matrix(1), preferred_element_type=F32
        )
        total[:part, :] += jnp.dot(
            views[ahead : ahead + part, :], matrix(0), preferred_element_type=F32
        )
        total[spread * half :, :] += jnp.dot(
            views[first : first + part, :], matrix(2), preferred_element_type=F32
        )
    width = FIRST_SPREAD
    for p in range(rows):
        at = pl.ds(p * half, half)
        value = early[p * cols : (p + 1) * cols, :] + jnp.concatenate(
            [low_total[at, :], high_total[at, :]], axis=0
        )
        value = jnp.where(pre[p].astype(F32) > 0, value, jnp.float32(0.0))
        local[p] = value.astype(BF16)
        edge_low[p * width : (p + 1) * width, :] = value[:width].astype(BF16)
        edge_high[p * width : (p + 1) * width, :] = value[cols - width :].astype(BF16)
    for r, span in enumerate(tap_rows(rows, half, spread, pad, -1)):
        side = {0: product(high_still, high_views, span), 2: product(low_still, low_views, span)}
        for c in range(3):
            k = 3 * r + c
            block = taps[k * chans : (k + 1) * chans, :]
            if c in side:
                block = block + side[c]
            place_tap(gradient, k, norm * block)
    hand_out(gradient, keep, send, segments)


def first_weight_kernel(
    norm, segments, inputs, low, high, local, keep, send, views, still, gradient
):
    rows, cols, chans = inputs.shape
    spread, pad = FIRST_SPREAD, FIRST_PAD
    build_views(inputs, low, high, views, spread, pad, 2, 0)
    still[...] = local[...].reshape(rows * cols, chans).T
    for r, span in enumerate(tap_rows(rows, cols, spread, pad, 1)):
        value = (norm * product(still, views, span)).astype(BF16)
        for c in range(3):
            block = value[:, c * chans : (c + 1) * chans].T
            place_tap(gradient, 3 * r + c, block.astype(F32))
    hand_out(gradient, keep, send, segments)


def first_input_kernel(local, low, high, weight, out, views, turned, total):
    rows, cols, chans = local.shape
    build_views(local, low, high, views, FIRST_SPREAD, 0, 0, 2)
    transpose_taps(weight, turned)
    input_side(views, turned, total, rows, cols, FIRST_SPREAD, 0)
    out[...] = total[...].astype(BF16).reshape(rows, cols, chans)


def edges_kernel(width, field, low, high):
    rows, cols, _ = field.shape
    for p in range(rows):
        row = field[p]
        low[p * width : (p + 1) * width, :] = row[:width]
        high[p * width : (p + 1) * width, :] = row[cols - width :]


def pair_kernel(keep, received, *outs):
    size = outs[0].shape[0]
    for m, out in enumerate(outs):
        at = pl.ds(m * size, size)
        out[...] = (keep[at, :].astype(F32) + received[at, :].astype(F32)).astype(BF16)


def chip_kernel(count, *refs):
    terms, own, pieces, level = refs[:count], refs[count], refs[count + 1 : -1], refs[-1]
    level[...] = sum((t[...].astype(F32) for t in terms[1:]), terms[0][...].astype(F32))
    size = own.shape[0]
    me = lax.axis_index("dp")

    def piece(m):
        start = pl.multiple_of(lax.bitwise_xor(me, m) * size, size)
        return level[pl.ds(start, size), :]

    own[...] = piece(0)
    for m, out in enumerate(pieces):
        out[...] = piece(m + 1).astype(BF16)


def last_kernel(own, *refs):
    refs[-1][...] = sum((t[...].astype(F32) for t in refs[:-1]), own[...])


def call(kernel, outs, scratch, *operands, limit=20, flops=0):
    whole = pl.BlockSpec(memory_space=pltpu.VMEM)
    return pl.pallas_call(
        kernel,
        out_shape=[jax.ShapeDtypeStruct(s, t) for s, t in outs],
        in_specs=[whole] * len(operands),
        out_specs=[whole] * len(outs),
        scratch_shapes=[pltpu.VMEM(s, t) for s, t in scratch],
        compiler_params=pltpu.CompilerParams(vmem_limit_bytes=limit * 2**20),
    )(*operands)


def ring(axis, step):
    count = lax.axis_size(axis)
    return [(i, (i + step) % count) for i in range(count)]


def swap(axis, mask):
    return [(i, i ^ mask) for i in range(lax.axis_size(axis))]


def exchange_edges(low_edge, high_edge):
    low = lax.ppermute(high_edge, "lon", ring("lon", 1))
    high = lax.ppermute(low_edge, "lon", ring("lon", -1))
    return low, high


def edges_of(field, width):
    shape = (field.shape[0] * width, field.shape[2])
    return call(functools.partial(edges_kernel, width), [(shape, BF16)] * 2, [], field, limit=4)


def reduce_partials(keep, send):
    chips = lax.axis_size("lon") // 2
    parts = lax.axis_size("dp")
    rows, lanes = keep.shape
    received = lax.ppermute(send, "lon", swap("lon", 1))
    piece = (rows // chips, lanes)
    paired = call(pair_kernel, [(piece, BF16)] * chips, [], keep, received, limit=4)
    arrived = [lax.ppermute(paired[m], "lon", swap("lon", 2 * m)) for m in range(1, chips)]
    small = (piece[0] // parts, lanes)
    own, *pieces = call(
        functools.partial(chip_kernel, chips),
        [(small, F32)] + [(small, BF16)] * (parts - 1),
        [(piece, F32)],
        paired[0], *arrived, limit=4,
    )
    arrived = [lax.ppermute(pieces[m - 1], "dp", swap("dp", m)) for m in range(1, parts)]
    (total,) = call(last_kernel, [(small, F32)], [], own, *arrived, limit=4)
    return total.reshape(-1)


def local(inputs, pre_act, cotangent, first_weight, second_weight):
    shape = inputs.shape
    inputs, pre_act, cotangent = (a.reshape(a.shape[1:]) for a in (inputs, pre_act, cotangent))
    rows, cols, chans = inputs.shape
    segments = lax.axis_size("lon")
    cells = rows * cols
    norm = float(shape[0] * cells * segments * lax.axis_size("dp")) ** -0.5
    taps = first_weight.shape[0]
    cot_low, cot_high = exchange_edges(*edges_of(cotangent, SECOND_SPREAD))
    in_low, in_high = exchange_edges(*edges_of(inputs, FIRST_SPREAD))
    matrix = (taps, chans)
    pieces = (taps, chans // 2)
    grid = (2 * taps, chans // 2)
    edge = (rows * FIRST_SPREAD, chans)
    side = (cells // 2, chans)
    early = call(
        second_early_kernel,
        [
            ((cells, chans), F32),
            (matrix, F32),
            (side[::-1], BF16),
            (side[::-1], BF16),
            (matrix, BF16),
        ],
        [(((rows + 2 * SECOND_PAD) * cols, 3 * chans), BF16), ((chans, cells), BF16)],
        pre_act, cotangent, second_weight,
    )
    strip = ((rows + 2 * SECOND_PAD) * cols // 2, chans)
    keep, send, local_grad, edge_low, edge_high = call(
        functools.partial(second_late_kernel, norm, segments),
        [(pieces, BF16), (pieces, BF16), ((rows, cols, chans), BF16), (edge, BF16), (edge, BF16)],
        [(strip, BF16), (strip, BF16), (side, F32), (side, F32), (grid, F32)],
        pre_act, cot_low, cot_high, *early,
    )
    second = reduce_partials(keep, send)
    keep, send = call(
        functools.partial(first_weight_kernel, norm, segments),
        [(pieces, BF16), (pieces, BF16)],
        [
            (((rows + 2 * FIRST_PAD) * cols, 3 * chans), BF16),
            ((chans, cells), BF16),
            (grid, F32),
        ],
        inputs, in_low, in_high, local_grad,
    )
    first = reduce_partials(keep, send)
    grad_low, grad_high = exchange_edges(edge_low, edge_high)
    (input_gradient,) = call(
        first_input_kernel,
        [((rows, cols, chans), BF16)],
        [((cells, 3 * chans), BF16), (matrix, BF16), ((cells, chans), F32)],
        local_grad, grad_low, grad_high, first_weight,
    )
    return input_gradient.reshape(shape), first, second


def solution(mesh):
    field = P("dp", None, "lon", None)
    return jax.shard_map(
        local,
        mesh=mesh,
        in_specs=(field, field, field, P(), P()),
        out_specs=(field, P(("lon", "dp")), P(("lon", "dp"))),
        check_vma=False,
    )
```

```python
import functools

import jax
import jax.numpy as jnp
from jax import lax
from jax.experimental import pallas as pl
from jax.experimental.pallas import tpu as pltpu
from jax.sharding import PartitionSpec as P


FIRST_SPREAD = 12
SECOND_SPREAD = 18
FIRST_PAD = 4
SECOND_PAD = 2
BF16 = jnp.bfloat16
F32 = jnp.float32


def moved_rows(row, low, high, spread):
    cols = row.shape[0]
    return (
        jnp.concatenate([row[spread:], high], axis=0).astype(BF16),
        jnp.concatenate([low, row[: cols - spread]], axis=0).astype(BF16),
    )


def build_views(src, low, high, views, spread, pad, plus, minus):
    rows, cols, chans = src.shape
    if pad:
        blank = jnp.zeros((pad * cols, 3 * chans), BF16)
        views[: pad * cols, :] = blank
        views[(pad + rows) * cols :, :] = blank
    for p in range(rows):
        at = pl.ds((pad + p) * cols, cols)
        row = src[p]
        views[at, chans : 2 * chans] = row
        row = row.astype(F32)
        if low is None:
            upper = lower = jnp.zeros((spread, chans), F32)
        else:
            strip = pl.ds(p * spread, spread)
            upper = high[strip, :].astype(F32)
            lower = low[strip, :].astype(F32)
        ahead, behind = moved_rows(row, lower, upper, spread)
        views[at, plus * chans : (plus + 1) * chans] = ahead
        views[at, minus * chans : (minus + 1) * chans] = behind


def transpose_taps(weight, turned):
    chans = weight.shape[1]
    for k in range(9):
        turned[k * chans : (k + 1) * chans, :] = weight[k * chans : (k + 1) * chans, :].T


def input_side(views, turned, total, rows, cols, spread, pad):
    part = (rows - spread) * cols
    first = pad * cols
    third = turned.shape[0] // 3
    total[...] = jnp.dot(
        views[first : first + rows * cols, :],
        turned[third : 2 * third, :],
        preferred_element_type=F32,
    )
    ahead = (pad + spread) * cols
    total[:part, :] += jnp.dot(
        views[ahead : ahead + part, :], turned[:third, :], preferred_element_type=F32
    )
    total[spread * cols :, :] += jnp.dot(
        views[first : first + part, :], turned[2 * third :, :], preferred_element_type=F32
    )


def tap_rows(rows, cols, spread, pad, direction):
    block = rows - spread + pad
    ahead = (0, block * cols, (pad + spread) * cols)
    middle = (0, rows * cols, pad * cols)
    behind = ((rows - block) * cols, rows * cols, 0)
    return (ahead, middle, behind) if direction < 0 else (behind, middle, ahead)


def product(still, views, span):
    low, high, start = span
    return jnp.dot(
        still[:, low:high], views[start : start + high - low, :], preferred_element_type=F32
    )


def place_tap(gradient, k, block):
    chans = block.shape[0]
    half = chans // 2
    for h in range(2):
        at = pl.ds(2 * k * chans + h, chans, stride=2)
        gradient[at, :] = block[:, h * half : (h + 1) * half]


def hand_out(gradient, keep, send, segments, parts, split):
    size = gradient.shape[0] // (segments * parts)
    chips = segments // 2
    place = lax.axis_index("lon")
    core = lax.rem(place, 2)
    chip = place // 2
    mine = lax.axis_index("dp")
    if split:
        order = [(m, n + low) for low in (0, 1) for m in range(chips) for n in range(0, parts, 2)]
    else:
        order = [(m, n) for m in range(chips) for n in range(parts)]
    for slot, (m, n) in enumerate(order):
        pair = 2 * lax.bitwise_xor(chip, m)
        part = lax.bitwise_xor(mine, n)
        to = pl.ds(slot * size, size)
        own = pl.multiple_of(((pair + core) * parts + part) * size, size)
        other = pl.multiple_of(((pair + 1 - core) * parts + part) * size, size)
        keep[to, :] = gradient[pl.ds(own, size), :]
        send[to, :] = gradient[pl.ds(other, size), :].astype(BF16)


def second_early_kernel(pre, cot, weight, total, taps, low_still, high_still, turned, views, still):
    rows, cols, chans = pre.shape
    spread, pad = SECOND_SPREAD, SECOND_PAD
    build_views(cot, None, None, views, spread, pad, 0, 2)
    transpose_taps(weight, turned)
    hidden = pre[...]
    hidden = jnp.maximum(hidden, jnp.zeros_like(hidden))
    still[...] = hidden.reshape(rows * cols, chans).T
    half = cols // 2
    low_still[...] = hidden[:, :half].reshape(rows * half, chans).T
    high_still[...] = hidden[:, half:].reshape(rows * half, chans).T
    input_side(views, turned, total, rows, cols, spread, pad)
    for r, span in enumerate(tap_rows(rows, cols, spread, pad, -1)):
        value = product(still, views, span)
        for c in range(3):
            k = 3 * r + c
            taps[k * chans : (k + 1) * chans, :] = value[:, c * chans : (c + 1) * chans]


def second_late_kernel(
    norm, segments, parts, pre, low, high, early, taps, low_still, high_still, turned,
    keep, send, local, edge_low, edge_high, low_views, high_views, low_total, high_total, gradient,
):
    rows, cols, chans = pre.shape
    spread, pad = SECOND_SPREAD, SECOND_PAD
    half = cols // 2
    blank = jnp.zeros((pad * half, chans), BF16)
    for views in (low_views, high_views):
        views[: pad * half, :] = blank
        views[(pad + rows) * half :, :] = blank
    gap = jnp.zeros((half - spread, chans), F32)
    for p in range(0, rows, 2):
        at = pl.ds((pad + p) * half, 2 * half)
        lower = [low[q * spread : (q + 1) * spread, :].astype(F32) for q in (p, p + 1)]
        upper = [high[q * spread : (q + 1) * spread, :].astype(F32) for q in (p, p + 1)]
        low_views[at, :] = jnp.concatenate([lower[0], gap, lower[1], gap], axis=0).astype(BF16)
        high_views[at, :] = jnp.concatenate([gap, upper[0], gap, upper[1]], axis=0).astype(BF16)

    part = (rows - spread) * half
    first = pad * half
    ahead = (pad + spread) * half
    for views, total, c in ((low_views, low_total, 2), (high_views, high_total, 0)):

        def matrix(r):
            k = 3 * r + c
            return turned[k * chans : (k + 1) * chans, :]

        total[...] = jnp.dot(
            views[first : first + rows * half, :], matrix(1), preferred_element_type=F32
        )
        total[:part, :] += jnp.dot(
            views[ahead : ahead + part, :], matrix(0), preferred_element_type=F32
        )
        total[spread * half :, :] += jnp.dot(
            views[first : first + part, :], matrix(2), preferred_element_type=F32
        )
    width = FIRST_SPREAD
    for p in range(rows):
        at = pl.ds(p * half, half)
        value = early[p * cols : (p + 1) * cols, :] + jnp.concatenate(
            [low_total[at, :], high_total[at, :]], axis=0
        )
        value = jnp.where(pre[p].astype(F32) > 0, value, jnp.float32(0.0))
        local[p] = value.astype(BF16)
        edge_low[p * width : (p + 1) * width, :] = value[:width].astype(BF16)
        edge_high[p * width : (p + 1) * width, :] = value[cols - width :].astype(BF16)
    for r, span in enumerate(tap_rows(rows, half, spread, pad, -1)):
        side = {0: product(high_still, high_views, span), 2: product(low_still, low_views, span)}
        for c in range(3):
            k = 3 * r + c
            block = taps[k * chans : (k + 1) * chans, :]
            if c in side:
                block = block + side[c]
            place_tap(gradient, k, norm * block)
    hand_out(gradient, keep, send, segments, parts, True)


def first_weight_kernel(
    norm, segments, parts, inputs, low, high, local, keep, send, views, still, gradient
):
    rows, cols, chans = inputs.shape
    spread, pad = FIRST_SPREAD, FIRST_PAD
    build_views(inputs, low, high, views, spread, pad, 2, 0)
    still[...] = local[...].reshape(rows * cols, chans).T
    for r, span in enumerate(tap_rows(rows, cols, spread, pad, 1)):
        value = (norm * product(still, views, span)).astype(BF16)
        for c in range(3):
            block = value[:, c * chans : (c + 1) * chans].T
            place_tap(gradient, 3 * r + c, block.astype(F32))
    hand_out(gradient, keep, send, segments, parts, False)


def first_input_kernel(local, low, high, weight, out, views, turned, total):
    rows, cols, chans = local.shape
    build_views(local, low, high, views, FIRST_SPREAD, 0, 0, 2)
    transpose_taps(weight, turned)
    input_side(views, turned, total, rows, cols, FIRST_SPREAD, 0)
    out[...] = total[...].astype(BF16).reshape(rows, cols, chans)


def edges_kernel(width, field, low, high):
    rows, cols, _ = field.shape
    for p in range(rows):
        row = field[p]
        low[p * width : (p + 1) * width, :] = row[:width]
        high[p * width : (p + 1) * width, :] = row[cols - width :]


def add_kernel(count, *refs):
    terms, outs = refs[:count], refs[count:]
    start = 0
    for out in outs:
        at = pl.ds(start, out.shape[0])
        total = terms[0][at, :].astype(F32)
        for term in terms[1:]:
            total = total + term[at, :].astype(F32)
        out[...] = total.astype(out.dtype)
        start += out.shape[0]


def call(kernel, outs, scratch, *operands, limit=20, flops=0):
    whole = pl.BlockSpec(memory_space=pltpu.VMEM)
    return pl.pallas_call(
        kernel,
        out_shape=[jax.ShapeDtypeStruct(s, t) for s, t in outs],
        in_specs=[whole] * len(operands),
        out_specs=[whole] * len(outs),
        scratch_shapes=[pltpu.VMEM(s, t) for s, t in scratch],
        compiler_params=pltpu.CompilerParams(vmem_limit_bytes=limit * 2**20),
    )(*operands)


def ring(axis, step):
    count = lax.axis_size(axis)
    return [(i, (i + step) % count) for i in range(count)]


def swap(axis, mask):
    return [(i, i ^ mask) for i in range(lax.axis_size(axis))]


def exchange_edges(low_edge, high_edge):
    low = lax.ppermute(high_edge, "lon", ring("lon", 1))
    high = lax.ppermute(low_edge, "lon", ring("lon", -1))
    return low, high


def edges_of(field, width):
    shape = (field.shape[0] * width, field.shape[2])
    return call(functools.partial(edges_kernel, width), [(shape, BF16)] * 2, [], field, limit=4)


def add(terms, counts, parts_rows):
    lanes = terms[0].shape[1]
    outs = [((c * parts_rows, lanes), BF16 if i else F32) for i, c in enumerate(counts)]
    kernel = functools.partial(add_kernel, len(terms))
    return call(kernel, outs, [], *terms, limit=6)


def move(axis, mask, value):
    return lax.ppermute(value, axis, swap(axis, mask))


def swaps(axis, masks, pieces):
    got = [move(axis, mask, piece) for mask, piece in reversed(list(zip(masks, pieces)))]
    return got[::-1]


def chip_masks(count):
    return range(2, count, 2)


def reduce_first(keep, send):
    segments, parts = lax.axis_size("lon"), lax.axis_size("dp")
    chips = segments // 2
    size = keep.shape[0] // (chips * parts)
    received = move("lon", 1, send)
    own, *others = add([keep, received], [parts] * chips, size)
    others = swaps("lon", chip_masks(segments), others)
    own, *others = add([own, *others], [1] * parts, size)
    others = swaps("dp", range(1, parts), others)
    (own,) = add([own, *others], [1], size)
    return own.reshape(-1)


def reduce_second(keep, send):
    segments, parts = lax.axis_size("lon"), lax.axis_size("dp")
    chips, half = segments // 2, parts // 2
    size = keep.shape[0] // (chips * parts)
    received = move("lon", 1, send)
    own, other = add([keep, received], [chips * half] * 2, size)
    received = move("dp", 1, other)
    own, *others = add([own, received], [half] * chips, size)
    others = swaps("lon", chip_masks(segments), others)
    own, *others = add([own, *others], [1] * half, size)
    others = swaps("dp", range(2, parts, 2), others)
    (own,) = add([own, *others], [1], size)
    return own.reshape(-1)


def local(inputs, pre_act, cotangent, first_weight, second_weight):
    shape = inputs.shape
    inputs, pre_act, cotangent = (a.reshape(a.shape[1:]) for a in (inputs, pre_act, cotangent))
    rows, cols, chans = inputs.shape
    segments, parts = lax.axis_size("lon"), lax.axis_size("dp")
    cells = rows * cols
    norm = float(shape[0] * cells * segments * parts) ** -0.5
    taps = first_weight.shape[0]
    cot_low, cot_high = exchange_edges(*edges_of(cotangent, SECOND_SPREAD))
    in_low, in_high = exchange_edges(*edges_of(inputs, FIRST_SPREAD))
    matrix = (taps, chans)
    pieces = (taps, chans // 2)
    grid = (2 * taps, chans // 2)
    edge = (rows * FIRST_SPREAD, chans)
    side = (cells // 2, chans)
    early = call(
        second_early_kernel,
        [
            ((cells, chans), F32),
            (matrix, F32),
            (side[::-1], BF16),
            (side[::-1], BF16),
            (matrix, BF16),
        ],
        [(((rows + 2 * SECOND_PAD) * cols, 3 * chans), BF16), ((chans, cells), BF16)],
        pre_act, cotangent, second_weight,
    )
    strip = ((rows + 2 * SECOND_PAD) * cols // 2, chans)
    keep, send, local_grad, edge_low, edge_high = call(
        functools.partial(second_late_kernel, norm, segments, parts),
        [(pieces, F32), (pieces, BF16), ((rows, cols, chans), BF16), (edge, BF16), (edge, BF16)],
        [(strip, BF16), (strip, BF16), (side, F32), (side, F32), (grid, F32)],
        pre_act, cot_low, cot_high, *early,
    )
    second = reduce_second(keep, send)
    keep, send = call(
        functools.partial(first_weight_kernel, norm, segments, parts),
        [(pieces, F32), (pieces, BF16)],
        [
            (((rows + 2 * FIRST_PAD) * cols, 3 * chans), BF16),
            ((chans, cells), BF16),
            (grid, F32),
        ],
        inputs, in_low, in_high, local_grad,
    )
    first = reduce_first(keep, send)
    grad_low, grad_high = exchange_edges(edge_low, edge_high)
    (input_gradient,) = call(
        first_input_kernel,
        [((rows, cols, chans), BF16)],
        [((cells, 3 * chans), BF16), (matrix, BF16), ((cells, chans), F32)],
        local_grad, grad_low, grad_high, first_weight,
    )
    return input_gradient.reshape(shape), first, second


def solution(mesh):
    field = P("dp", None, "lon", None)
    return jax.shard_map(
        local,
        mesh=mesh,
        in_specs=(field, field, field, P(), P()),
        out_specs=(field, P(("lon", "dp")), P(("lon", "dp"))),
        check_vma=False,
    )
```
